256 devices in a mesh: section: 2 (over core), dp: 16 (over z, x_lo), tensor: 8 (over y, x_hi).
Axes of the slice: x: 4 (x_hi: 2, x_lo: 2; x = x_hi * 2 + x_lo), y: 4, z: 8, core: 2. Of those that a mesh axis runs over, the one named last changes fastest.
Arguments:
- tokens: bfloat16 [2048, 4096], P('dp', 'tensor'), may hold values from -6 to 6
- gain: bfloat16 [2, 4096], P('section', 'tensor'), may hold values from 0.099609375 to 1.8984375
- w_up: bfloat16 [2, 4096, 5120], P('section', 'dp', 'tensor'), may hold values from -0.09375 to 0.09375
- w_down: bfloat16 [2, 5120, 4096], P('section', 'tensor', 'dp'), may hold values from -0.078125 to 0.078125
- cotangent: bfloat16 [2, 2048, 4096], P('section', 'dp'), may hold values from -6 to 6
Outputs:
- states: bfloat16 [2, 2048, 4096], P('section', 'dp', 'tensor')
- grad_down: bfloat16 [2, 5120, 4096], P('section', 'tensor', 'dp')
The draws below stay inside these ranges and needn't reach their ends.
All inputs are finite; a program needn't handle non-finite values.
Results may differ from the reference program's by a relative error of at most 0.02.
Values may be sent and summed in bfloat16 or wider, within the bound.
No kernel may reach another device: no remote copies, remote signals or barrier semaphores. Data moves between devices by JAX's collectives and lax.ppermute only.
A program may use at most 64 MiB of HBM per device.

```python
import jax
import jax.numpy as jnp
from jax import lax

WIDTH = 4096
HIDDEN_SIZE = 5120
TOK_DEV = 128
TOKENS = 2048
LAYERS = 2
N_SECTION = 2
N_DP = 16
N_TENSOR = 8


def block_levels(own_key, dims, pieces, low, high):
    level = 1.0
    for dim, blocks in pieces:
        steps = jax.random.uniform(jax.random.fold_in(jax.random.fold_in(own_key, 6), dim), (blocks,), jnp.float32, low / len(pieces), high / len(pieces))
        level = level * jnp.repeat(jnp.exp(steps), dims[dim] // blocks).reshape((-1,) + (1,) * (len(dims) - 1 - dim))
    return level


def normal_values(key, extent, deviation, bound, cuts=(), dtype=jnp.bfloat16):
    drawn = deviation * jax.random.normal(key, extent, jnp.float32)
    if cuts:
        drawn = drawn * block_levels(key, extent, cuts, -0.22, 0.18)
    return jnp.clip(drawn, -bound, bound).astype(dtype)


def setup_inputs(seed: int = 0) -> dict:
    arg_keys = jax.random.split(jax.random.key(seed), 6)
    return {
        "tokens": normal_values(arg_keys[0], (TOKENS, WIDTH), 1.0, 6.0, ((0, 16), (1, 8))),
        "gain": jnp.clip(1.0 + 0.18 * jax.random.normal(arg_keys[1], (LAYERS, WIDTH), jnp.float32), 0.099609375, 1.8984375).astype(jnp.bfloat16),
        "w_up": normal_values(arg_keys[2], (LAYERS, WIDTH, HIDDEN_SIZE), WIDTH ** -0.5, 0.09375, ((0, 2), (1, 16), (2, 8))),
        "w_down": normal_values(arg_keys[3], (LAYERS, HIDDEN_SIZE, WIDTH), HIDDEN_SIZE ** -0.5, 0.078125, ((0, 2), (1, 8), (2, 16))),
        "cotangent": normal_values(arg_keys[4], (LAYERS, TOKENS, WIDTH), 1.0, 6.0, ((0, 2), (1, 16))),
    }


EPS = 1e-06

def layer_ref(acts, gain_row, up_mat, down_mat):
    acts_f = acts.astype(jnp.float32)
    mean_sq = lax.optimization_barrier(jnp.mean(acts_f * acts_f, axis=1, keepdims=True))
    normed = (acts_f * lax.rsqrt(mean_sq + EPS) * gain_row.astype(jnp.float32)).astype(jnp.bfloat16)
    pre_act = jnp.dot(normed, up_mat, preferred_element_type=jnp.float32)
    hidden = jax.nn.gelu(pre_act, approximate=True).astype(jnp.bfloat16)
    group_width = HIDDEN_SIZE // N_TENSOR
    summed = jnp.zeros(acts.shape, jnp.float32)
    for group_id in range(N_TENSOR):
        lower = group_id * group_width
        partial_value = jnp.dot(hidden[:, lower:lower + group_width], down_mat[lower:lower + group_width, :], preferred_element_type=jnp.float32).astype(jnp.bfloat16)
        summed = summed + lax.optimization_barrier(partial_value).astype(jnp.float32)
    return ((acts_f + summed).astype(jnp.bfloat16), hidden)

def reference(tokens, gain, w_up, w_down, cotangent):
    acts = tokens
    states = []
    grads = []
    for layer_id in range(N_SECTION):
        acts, hidden = layer_ref(acts, gain[layer_id], w_up[layer_id], w_down[layer_id])
        states.append(acts)
        grad_sum = jnp.zeros((HIDDEN_SIZE, WIDTH), jnp.float32)
        for peer_id in range(N_DP):
            lower = peer_id * TOK_DEV
            partial_value = lax.dot_general(hidden[lower:lower + TOK_DEV], cotangent[layer_id][lower:lower + TOK_DEV], (((0,), (0,)), ((), ())), preferred_element_type=jnp.float32).astype(jnp.bfloat16)
            grad_sum = grad_sum + lax.optimization_barrier(partial_value).astype(jnp.float32)
        grads.append(grad_sum.astype(jnp.bfloat16))
    return (jnp.stack(states), jnp.stack(grads))
```

```python
import itertools

import jax
import jax.numpy as jnp
from jax import lax
from jax.experimental import pallas as pl
from jax.experimental.pallas import tpu as pltpu
from jax.sharding import Mesh
from jax.sharding import PartitionSpec as P


EPS = 1e-06
BF = jnp.bfloat16
F32 = jnp.float32
AXES = ("c", "zh", "zl", "xl", "y", "xh")
SIZES = (2, 4, 2, 2, 4, 2)
DP = ("zh", "zl", "xl")
TP = ("y", "xh")
C, ZH, ZL, XL, Y, XH = range(6)
TAIL = 128


def flat(place):
    number = 0
    for at, size in zip(place, SIZES):
        number = number * size + at
    return number


def moved(array, to):
    places = itertools.product(*(range(size) for size in SIZES))
    pairs = [(flat(place), flat(to(*place))) for place in places]
    return lax.ppermute(array, AXES, pairs)


def over_core(array):
    return moved(array, lambda c, zh, zl, xl, y, xh: (1 - c, zh, zl, xl, y, xh))


def over_pair(array):
    return moved(array, lambda c, zh, zl, xl, y, xh: (c, zh, 1 - zl, xl, y, xh))


def over_x(array, s):
    return moved(
        array, lambda c, zh, zl, xl, y, xh: (c, zh, zl, xl ^ (s & 1), y, xh ^ (s >> 1))
    )


def over_y(array, s):
    return moved(array, lambda c, zh, zl, xl, y, xh: (c, zh, zl, xl, y ^ s, xh))


def over_zh(array, s):
    return moved(array, lambda c, zh, zl, xl, y, xh: (c, zh ^ s, zl, xl, y, xh))


def turned(array, q, r):
    return moved(array, lambda c, zh, zl, xl, y, xh: (c ^ q, y, zl, xl, zh, xh ^ r))


def call(kernel, outs, scratch, flops, *operands):
    smem = pl.BlockSpec(memory_space=pltpu.SMEM)
    vmem = pl.BlockSpec(memory_space=pltpu.VMEM)
    size = sum(a.size * a.dtype.itemsize for a in (*operands, *outs))
    return pl.pallas_call(
        kernel,
        out_shape=outs,
        in_specs=[smem] + [vmem] * (len(operands) - 1),
        out_specs=[vmem] * len(outs),
        scratch_shapes=scratch,
        cost_estimate=pl.CostEstimate(
            flops=flops, bytes_accessed=int(size), transcendentals=0
        ),
    )(*operands)


def up_kernel(at, gain, *refs):
    xs, own, other, outs = refs[:4], refs[4:8], refs[8:12], refs[12:16]
    x_all, weights, stats = refs[16:]
    for s in range(4):
        half = at[XH] ^ (s >> 1)
        for a in range(2):
            row = 512 * (at[ZL] ^ a) + 256 * (at[XL] ^ (s & 1))
            row_own = pl.multiple_of(row + 128 * at[C], 128)
            row_other = pl.multiple_of(row + 128 * (1 - at[C]), 128)
            weights[half, pl.ds(row_own, 128), :] = own[s][a]
            weights[half, pl.ds(row_other, 128), :] = other[s][a]
    gain_f = gain[0:1, :].astype(F32)
    lane = lax.broadcasted_iota(jnp.int32, (32, TAIL), 1)
    for p in range(4):
        slot = at[Y] ^ at[ZH] ^ p
        x = xs[p][...].astype(F32)
        x_all[pl.ds(pl.multiple_of(32 * slot, 32), 32), :] = (x * gain_f).astype(BF)
        total = jnp.sum(x * x, axis=1, keepdims=True)
        high = total.astype(BF).astype(F32)
        low = total - high
        tail = jnp.where(lane == 0, high, jnp.where(lane == 1, low, 0.0))
        stats[slot] = tail.astype(BF)
    for half in range(2):
        product = jnp.dot(x_all[...], weights[half], preferred_element_type=F32)
        for s in range(4):
            outs[s][:, 640 * half : 640 * half + 640] = product[32 * s : 32 * s + 32].astype(BF)
    for s in range(4):
        outs[s][:, 1280:] = stats[s]


def gelu_kernel(at, *refs):
    parts, out = refs[:4], refs[4]
    tail = sum(part[:, 1280:].astype(F32) for part in parts)
    mean_sq = (tail[:, 0:1] + tail[:, 1:2]) * (1.0 / 4096)
    inverse_rms = lax.rsqrt(mean_sq + EPS)
    pre_act = sum(part[:, :1280].astype(F32) for part in parts) * inverse_rms
    out[...] = jax.nn.gelu(pre_act, approximate=True).astype(BF)


def down_kernel(at, *refs):
    hs, own, other, outs = refs[:4], refs[4:8], refs[8:12], refs[12:16]
    h_all, weights = refs[16:]
    for s in range(4):
        row = pl.multiple_of(640 * (at[XH] ^ (s >> 1)), 128)
        for a in range(2):
            block = 4 * (at[ZL] ^ a) + 2 * (at[XL] ^ (s & 1))
            weights[block + at[C], pl.ds(row, 640), :] = own[s][a]
            weights[block + 1 - at[C], pl.ds(row, 640), :] = other[s][a]
    for p in range(4):
        slot = at[Y] ^ at[ZH] ^ p
        h_all[pl.ds(pl.multiple_of(32 * slot, 32), 32), :] = hs[p][...]
    for block in range(4):
        columns = jnp.concatenate([weights[2 * block], weights[2 * block + 1]], axis=1)
        product = jnp.dot(h_all[...], columns, preferred_element_type=F32)
        for s in range(4):
            outs[s][:, 256 * block : 256 * block + 256] = product[32 * s : 32 * s + 32].astype(BF)


def grad_kernel(at, *refs):
    here, there, cots, outs = refs[:2], refs[2:4], refs[4:8], refs[8:12]
    h_all, c_all = refs[12:]
    for core, pair in ((at[C], here), (1 - at[C], there)):
        row = pl.multiple_of(32 * core, 32)
        for a in range(2):
            for p in range(4):
                z = 2 * (at[ZH] ^ p) + (at[ZL] ^ a)
                block = pair[a][32 * p : 32 * p + 32, :]
                h_all[0, z, pl.ds(row, 32), :] = block[:, :640]
                h_all[1, z, pl.ds(row, 32), :] = block[:, 640:]
    for s in range(4):
        row = pl.multiple_of(16 * (at[Y] ^ s), 16)
        for z in range(8):
            left, right = cots[s][z, :, :256], cots[s][z, :, 256:]
            c_all[at[XL], z, pl.ds(row, 16), :] = left
            c_all[1 - at[XL], z, pl.ds(row, 16), :] = right
    for j in range(2):
        turned_h = h_all[at[XH] ^ j].reshape(512, 640).T
        for i in range(2):
            product = jnp.dot(turned_h, c_all[i].reshape(512, 256), preferred_element_type=F32)
            outs[2 * j + i][...] = product.astype(BF)


def body(tokens, gain, w_up, w_down, cotangent):
    c, zh, zl, xl, y, xh = (lax.axis_index(name) for name in AXES)
    at = jnp.stack([c, zh, zl, xl, y, xh]).astype(jnp.int32)
    shape = jax.ShapeDtypeStruct

    def pick(flag, first, second):
        return jnp.where(flag == 0, first, second)

    gain_rows = jnp.broadcast_to(gain, (16, 512))

    def entry(r):
        rows = lax.dynamic_slice_in_dim(tokens, 64 * (xh ^ r) + 32 * c, 32, 0)
        return turned(jnp.concatenate([rows, gain_rows], axis=0), 0, r)

    def by_core(array, dim):
        own = lax.dynamic_slice_in_dim(array, 128 * c, 128, dim)
        other = over_core(lax.dynamic_slice_in_dim(array, 128 * (1 - c), 128, dim))
        return (pick(c, own, other), pick(c, other, own))

    def gathered(half):
        pair = jnp.stack([half, over_pair(half)])
        own = [pair] + [over_x(pair, s) for s in (1, 2, 3)]
        return own + [over_core(piece) for piece in own]

    up_halves = by_core(w_up[0], 0)
    entered = [entry(0), entry(1)]
    down_halves = by_core(w_down[0], 1)
    entered = pick(
        xh, jnp.concatenate(entered, axis=1), jnp.concatenate(entered[::-1], axis=1)
    )
    acts = entered[:32]
    gain_own = entered[32:]
    gain_other = over_core(gain_own)
    gains = (pick(c, gain_own, gain_other), pick(c, gain_other, gain_own))

    cot_rows = lax.dynamic_slice_in_dim(cotangent[0], 64 * xh + 16 * y, 16, 0)
    cot_split = jnp.moveaxis(cot_rows.reshape(16, 8, 512), 1, 0)
    cot_mine = lax.all_to_all(cot_split, ("zh", "zl"), 0, 0, tiled=True)
    cots = [cot_mine] + [over_y(cot_mine, s) for s in (1, 2, 3)]

    states = []
    hiddens = []
    for layer in range(2):
        up = gathered(up_halves[layer])
        down = gathered(down_halves[layer])
        pieces = [acts] + [over_y(acts, s) for s in (1, 2, 3)]
        sums = call(
            up_kernel,
            [shape((32, 1280 + TAIL), BF)] * 4,
            [
                pltpu.VMEM((128, 1024), BF),
                pltpu.VMEM((2, 1024, 640), BF),
                pltpu.VMEM((4, 32, TAIL), BF),
            ],
            2 * 128 * 1024 * 1280,
            at,
            gains[layer],
            *pieces,
            *up,
        )
        sums = [sums[0]] + [over_zh(sums[s], s) for s in (1, 2, 3)]
        (hidden,) = call(gelu_kernel, [shape((32, 1280), BF)], [], 32 * 1280 * 20, at, *sums)
        pieces = [hidden] + [over_zh(hidden, s) for s in (1, 2, 3)]
        sums = call(
            down_kernel,
            [shape((32, 1024), BF)] * 4,
            [pltpu.VMEM((128, 1280), BF), pltpu.VMEM((8, 1280, 128), BF)],
            2 * 128 * 1024 * 1280,
            at,
            *pieces,
            *down,
        )
        arrived = [sums[0]] + [over_y(sums[s], s) for s in (1, 2, 3)]
        summed = sum(part.astype(F32) for part in arrived)
        acts = (acts.astype(F32) + summed).astype(BF)
        states.append(acts)
        block = jnp.concatenate(pieces, axis=0)
        hiddens.append([block, over_pair(block)])

    here = [pick(c, hiddens[0][a], hiddens[1][a]) for a in range(2)]
    there = [over_core(pick(c, hiddens[1][a], hiddens[0][a])) for a in range(2)]
    shares = call(
        grad_kernel,
        [shape((640, 256), BF)] * 4,
        [pltpu.VMEM((2, 8, 64, 640), BF), pltpu.VMEM((2, 8, 64, 256), BF)],
        2 * 512 * 1280 * 512,
        at,
        *here,
        *there,
        *cots,
    )
    arrived = [shares[0]] + [over_x(shares[s], s) for s in (1, 2, 3)]
    grad = sum(part.astype(F32) for part in arrived).astype(BF)

    def leave(q, r):
        chosen = pick(c ^ q, states[0], states[1])
        return turned(lax.dynamic_slice_in_dim(chosen, 512 * (xh ^ r), 512, 1), q, r)

    left = [[leave(q, r) for q in range(2)] for r in range(2)]
    blocks = [
        pick(c, jnp.concatenate(row, axis=0), jnp.concatenate(row[::-1], axis=0)) for row in left
    ]
    state = pick(
        xh, jnp.concatenate(blocks, axis=0), jnp.concatenate(blocks[::-1], axis=0)
    )
    return (state[None], grad[None])


def solution(mesh):
    torus = Mesh(mesh.devices.reshape(SIZES), AXES)
    in_specs = (P(DP, TP), P("c", TP), P("c", DP, TP), P("c", TP, DP), P("c", DP, None))
    out_specs = (P("c", DP, TP), P("c", TP, DP))
    return jax.shard_map(body, mesh=torus, in_specs=in_specs, out_specs=out_specs, check_vma=False)
```
